32 devices in a mesh: blk: 16 (over z, y, core), row: 2 (over x).
Axes of the slice: x: 2, y: 2, z: 4, core: 2. Of those that a mesh axis runs over, the one named last changes fastest.
Arguments:
- features: float32 [2048, 256], P(('blk', 'row')), may hold values from -2 to 2, as said below
- probes: float32 [2048, 128], P(('blk', 'row')), may hold values from -6 to 6
- outputscale: float32 [1], replicated, may hold values from 0.05 to 0.2
- noise: float32 [1], replicated, may hold values from 0.5 to 2
- pivots: int32 [256], replicated, may hold values from 0 to 2047, as said below
Outputs:
- product: float32 [2048, 128], P(('blk', 'row'))
- preconditioned: float32 [2048, 128], P(('blk', 'row'))
The draws below stay inside these ranges and needn't reach their ends.
Inputs may be any that keep to these rules, and one draw needn't show every extreme that they name: `pivots`: 256 distinct point indices. real-valued features.
All inputs are finite; a program needn't handle non-finite values.
Results may differ from the reference program's by a relative error of at most 0.0003.
Values sent between devices are 32-bit elements; how exact they have to be, the bound alone decides.
No kernel may reach another device: no remote copies, remote signals or barrier semaphores. Data moves between devices by JAX's collectives and lax.ppermute only.
A program may use at most 64 MiB of HBM per device.

```python
import math
import jax
import jax.numpy as jnp
from jax import lax

F = 256
PROBES = 128
RANK = 256
POINTS = 2048


def draw_pivots(key, part):
    ordering = jax.random.permutation(jax.random.fold_in(key, 7), POINTS)
    return ordering[:RANK].astype(jnp.int32)


def draw_features(key, part):
    key_list = [jax.random.fold_in(key, 101 + position) for position in range(7)]
    centres = 0.8 * jnp.clip(jax.random.normal(key_list[0], (64, 8), jnp.float32), -3.0, 3.0)
    owners = jax.random.randint(key_list[1], (POINTS,), 0, 64)
    offsets = jnp.clip(jax.random.normal(key_list[2], (POINTS, 8), jnp.float32), -3.0, 3.0)
    spread = jnp.exp(jax.random.uniform(key_list[3], (POINTS, 1), jnp.float32, math.log(0.15), math.log(0.6)))
    jitter = jnp.clip(jax.random.normal(key_list[6], (POINTS, F), jnp.float32), -4.0, 4.0)
    latent = centres[owners] + spread * offsets
    mixing = jnp.clip(jax.random.normal(key_list[4], (8, F), jnp.float32), -4.0, 4.0) / math.sqrt(F)
    bending = jnp.clip(jax.random.normal(key_list[5], (8, F), jnp.float32), -4.0, 4.0) / math.sqrt(8.0)
    linear_part = jnp.dot(latent, mixing, precision=lax.Precision.HIGHEST, preferred_element_type=jnp.float32)
    curved_part = jnp.tanh(jnp.dot(latent, bending, precision=lax.Precision.HIGHEST, preferred_element_type=jnp.float32))
    result_feats = linear_part + 0.7 / math.sqrt(F) * curved_part + 0.34 / math.sqrt(F) * jitter
    return jnp.clip(result_feats, -2.0, 2.0).astype(jnp.float32)


def steps_of(own_key, extent, shards, smallest, top_value):
    def one(dim, shards_of):
        steps = jax.random.uniform(jax.random.fold_in(jax.random.fold_in(own_key, 6), dim), (shards_of,), jnp.float32, smallest / len(shards), top_value / len(shards))
        return jnp.repeat(jnp.exp(steps), extent[dim] // shards_of).reshape((-1,) + (1,) * (len(extent) - dim - 1))

    level = one(*shards[0])
    for cut in shards[1:]:
        level = level * one(*cut)
    return level


def normal_values(own_key, shape, scale, limit, shards=(), held_as=jnp.bfloat16):
    drawn = scale * jax.random.normal(own_key, shape, jnp.float32)
    if shards:
        drawn = drawn * steps_of(own_key, shape, shards, -0.22, 0.18)
    return jnp.clip(drawn, -limit, limit).astype(held_as)


def setup_inputs(seed: int = 0) -> dict:
    key_of = jax.random.split(jax.random.key(seed), 6)
    return {
        "features": draw_features(jax.random.fold_in(key_of[5], 71), 0),
        "probes": normal_values(key_of[1], (POINTS, PROBES), 1.0, 6.0, ((0, 32),), jnp.float32),
        "outputscale": jnp.clip(jnp.exp(jax.random.uniform(key_of[2], (1,), jnp.float32, math.log(0.05), math.log(0.2))), 0.05, 0.2),
        "noise": jnp.clip(jnp.exp(jax.random.uniform(key_of[3], (1,), jnp.float32, math.log(0.5), math.log(2.0))), 0.5, 2.0),
        "pivots": draw_pivots(jax.random.fold_in(key_of[5], 71), 0),
    }


highest = lax.Precision.HIGHEST
root_five = 2.23606797749979

def kernel_tile(row_feats, row_norms, col_feats, col_norms):
    inner = lax.dot_general(row_feats.astype(jnp.float32), col_feats.astype(jnp.float32), (((1,), (1,)), ((), ())), precision=highest, preferred_element_type=jnp.float32)
    squared = jnp.maximum(row_norms[:, None] + col_norms[None, :] - 2.0 * inner, 0.0)
    scaled = root_five * jnp.sqrt(squared)
    return (1.0 + scaled + scaled * scaled / 3.0) * jnp.exp(-scaled)

def reference(features, probes, outputscale, noise, pivots):
    total_points, feature_count = features.shape
    amplitude = outputscale[0]
    nugget = noise[0]
    norms = lax.optimization_barrier(jnp.sum(features * features, axis=1))
    span = math.gcd(total_points, 1024)

    def one_block(inputs):
        block_feats, block_norms = inputs
        kernel_block = kernel_tile(block_feats, block_norms, features, norms)
        return jnp.dot(kernel_block.astype(jnp.float32), probes.astype(jnp.float32), precision=highest, preferred_element_type=jnp.float32)
    kernel_probes = lax.map(one_block, (features.reshape(-1, span, feature_count), norms.reshape(-1, span)))
    kernel_probes = kernel_probes.reshape(total_points, -1)
    product = amplitude * kernel_probes + nugget * probes
    pivot_feats = features[pivots]
    pivot_norms = lax.optimization_barrier(jnp.sum(pivot_feats * pivot_feats, axis=1))
    cross = amplitude * kernel_tile(features, norms, pivot_feats, pivot_norms)
    inner_pivots = amplitude * kernel_tile(pivot_feats, pivot_norms, pivot_feats, pivot_norms)
    gram = nugget * inner_pivots + lax.dot_general(cross.astype(jnp.float32), cross.astype(jnp.float32), (((0,), (0,)), ((), ())), precision=highest, preferred_element_type=jnp.float32)
    projected = lax.dot_general(cross.astype(jnp.float32), product.astype(jnp.float32), (((0,), (0,)), ((), ())), precision=highest, preferred_element_type=jnp.float32)
    factor = jnp.linalg.cholesky(gram)
    coefficients = jax.scipy.linalg.cho_solve((factor, True), projected)
    preconditioned = (product - jnp.dot(cross.astype(jnp.float32), coefficients.astype(jnp.float32), precision=highest, preferred_element_type=jnp.float32)) / nugget
    return (product, preconditioned)
```

```python
import functools

import jax
import jax.numpy as jnp
from jax import lax
from jax.experimental import pallas as pl
from jax.experimental.pallas import tpu as pltpu
from jax.sharding import PartitionSpec as P

highest = lax.Precision.HIGHEST
root_five = 2.23606797749979
tiny = 1e-30
AXES = ("blk", "row")
NT = (((1,), (1,)), ((), ()))
NN = (((1,), (0,)), ((), ()))


def split(value):
    high = value.astype(jnp.bfloat16)
    low = (value - high.astype(jnp.float32)).astype(jnp.bfloat16)
    return high, low


def dot3(left, right, dims):
    left_high, left_low = left
    right_high, right_low = right
    product = functools.partial(
        lax.dot_general, dimension_numbers=dims, preferred_element_type=jnp.float32
    )
    return (
        product(left_high, right_low) + product(left_low, right_high) + product(left_high, right_high)
    )


def dot6(left, right, dims):
    return lax.dot_general(left, right, dims, precision=highest, preferred_element_type=jnp.float32)


def matern(row_feats, row_norms, col_feats, col_norms):
    five_squared = dot6(row_feats, col_feats, NT) + row_norms + col_norms
    five_squared = jnp.maximum(five_squared, tiny)
    scaled = five_squared * lax.rsqrt(five_squared)
    return (1.0 + scaled + five_squared * (1.0 / 3.0)) * jnp.exp(-scaled)


def lane_norms(feats):
    ones = jnp.full((8, feats.shape[1]), 5.0, jnp.float32)
    return dot6(ones, feats * feats, NT)[0:1, :]


def tile_kernel(index_ref, scalar_ref, *refs):
    pieces = refs[:8]
    probes_ref, gram_ref, send_ref, keep_ref, cross_ref, all_ref, query_ref = refs[8:]
    line_rows, feature_count = pieces[0].shape
    rank = gram_ref.shape[0]
    local_rows = cross_ref.shape[0]
    amplitude = scalar_ref[0]
    nugget = scalar_ref[1]
    for position, piece in enumerate(pieces):
        all_ref[position * line_rows : (position + 1) * line_rows, :] = piece[:, :]

    def pick(step, carry):
        query_ref[pl.ds(step, 1), :] = all_ref[pl.ds(index_ref[step], 1), :]
        return carry

    lax.fori_loop(0, rank, pick, 0, unroll=8)
    pivot_feats = query_ref[:rank, :]
    line_feats = pieces[0][:, :]
    query_ref[rank:, :] = line_feats
    query = query_ref[:, :]
    query_norms = 5.0 * jnp.sum(query * query, axis=1, keepdims=True)
    query_scaled = -10.0 * query
    pivot_norms = lane_norms(pivot_feats)
    line_norms = lane_norms(line_feats)
    probes = split(probes_ref[:, :])
    total = None
    line_cross = None
    for position, piece in enumerate(pieces):
        feats = piece[:, :]
        tile = matern(query_scaled, query_norms, feats, lane_norms(feats))
        halves = split(tile)
        part = dot3((halves[0][:rank], halves[1][:rank]), halves, NT)
        total = part if total is None else total + part
        if position == 0:
            line_cross = tile[:rank, :]
        own = feats[:local_rows, :]
        own_norms = 5.0 * jnp.sum(own * own, axis=1, keepdims=True)
        own_tile = matern(-10.0 * own, own_norms, line_feats, line_norms)
        rows = dot3(split(own_tile), probes, NN)
        if position < 4:
            keep_ref[position * local_rows : (position + 1) * local_rows, :] = rows
        else:
            send_ref[(position - 4) * local_rows : (position - 3) * local_rows, :] = rows
        if position == 0:
            cross_ref[:, :] = amplitude * matern(-10.0 * own, own_norms, pivot_feats, pivot_norms)
    inner = matern(query_scaled[:rank], query_norms[:rank], pivot_feats, pivot_norms)
    square = amplitude * amplitude
    gram_ref[:, :] = (nugget * amplitude) * inner + square * total[:, :rank]
    mixed = square * total[:, rank:] + (nugget * amplitude) * line_cross
    projected = dot3(split(mixed), probes, NN)
    keep_ref[4 * local_rows :, :] = projected
    send_ref[4 * local_rows :, :] = projected


def exchanged(value, mask, count):
    return lax.ppermute(value, AXES, [(i, i ^ mask) for i in range(count)])


def small_slice(features, probes, outputscale, noise, pivots):
    local_rows, probe_count = probes.shape
    feature_count = features.shape[1]
    rank = pivots.shape[0]
    row_count = lax.axis_size("row")
    count = lax.axis_size("blk") * row_count
    flat_index = lax.axis_index("blk") * row_count + lax.axis_index("row")
    step_x, step_core, step_y, step_z = 1, row_count, 2 * row_count, 4 * row_count
    send = functools.partial(exchanged, count=count)

    owner = (pivots // local_rows) ^ flat_index
    slot = (owner & 1) + 2 * ((owner // step_y) & 1) + 4 * ((owner // step_core) & 1)
    index = (slot * 4 + owner // step_z) * local_rows + pivots % local_rows

    packed = jnp.concatenate([features, probes], axis=1)
    line = [packed] + [send(packed, step_z * step) for step in (1, 2, 3)]
    line_feats = jnp.concatenate([part[:, :feature_count] for part in line], axis=0)
    line_probes = jnp.concatenate([part[:, feature_count:] for part in line], axis=0)
    pieces = [line_feats] + [send(line_feats, mask) for mask in (step_x, step_y, step_x + step_y)]
    pieces = pieces + [send(piece, step_core) for piece in pieces]

    vmem = pl.BlockSpec(memory_space=pltpu.VMEM)
    smem = pl.BlockSpec(memory_space=pltpu.SMEM)
    half = 4 * local_rows + rank
    gram, outgoing, kept, cross = pl.pallas_call(
        tile_kernel,
        out_shape=(
            jax.ShapeDtypeStruct((rank, rank), jnp.float32),
            jax.ShapeDtypeStruct((half, probe_count), jnp.float32),
            jax.ShapeDtypeStruct((half, probe_count), jnp.float32),
            jax.ShapeDtypeStruct((local_rows, rank), jnp.float32),
        ),
        in_specs=[smem, smem] + [vmem] * 9,
        out_specs=(vmem,) * 4,
        scratch_shapes=[
            pltpu.VMEM((8 * 4 * local_rows, feature_count), jnp.float32),
            pltpu.VMEM((rank + 4 * local_rows, feature_count), jnp.float32),
        ],
        name="tiles",
    )(index, jnp.concatenate([outputscale, noise]), *pieces, line_probes)

    amplitude = outputscale[0]
    nugget = noise[0]
    kept = kept + send(outgoing, step_core)
    part = lambda position: kept[position * local_rows : (position + 1) * local_rows]
    projected = kept[4 * local_rows :]
    arrived = send(jnp.concatenate([part(1), part(3), projected]), step_x)
    first = part(0) + arrived[:local_rows]
    third = part(2) + arrived[local_rows : 2 * local_rows]
    projected = projected + arrived[2 * local_rows :]
    arrived = send(jnp.concatenate([third, projected]), step_y)
    product = amplitude * (first + arrived[:local_rows]) + nugget * probes
    projected = projected + arrived[local_rows:]
    factor = jnp.linalg.cholesky(gram)
    coefficients = jax.scipy.linalg.cho_solve((factor, True), projected)
    correction = jnp.dot(cross, coefficients, precision=highest, preferred_element_type=jnp.float32)
    return product, (product - correction) / nugget


def plain_tile(row_feats, col_feats):
    row_norms = 5.0 * jnp.sum(row_feats * row_feats, axis=1)[:, None]
    col_norms = 5.0 * jnp.sum(col_feats * col_feats, axis=1)[None, :]
    return matern(-10.0 * row_feats, row_norms, col_feats, col_norms)


def large_slice(features, probes, outputscale, noise, pivots):
    dot = functools.partial(jnp.dot, precision=highest, preferred_element_type=jnp.float32)
    amplitude = outputscale[0]
    nugget = noise[0]
    all_feats = lax.all_gather(features, AXES, axis=0, tiled=True)
    all_probes = lax.all_gather(probes, AXES, axis=0, tiled=True)
    product = amplitude * dot(plain_tile(features, all_feats), all_probes) + nugget * probes
    pivot_feats = all_feats[pivots]
    cross = amplitude * plain_tile(features, pivot_feats)
    inner = amplitude * plain_tile(pivot_feats, pivot_feats)
    gram, projected = lax.psum((dot(cross.T, cross), dot(cross.T, product)), AXES)
    factor = jnp.linalg.cholesky(nugget * inner + gram)
    coefficients = jax.scipy.linalg.cho_solve((factor, True), projected)
    return product, (product - dot(cross, coefficients)) / nugget


def solution(mesh):
    small = mesh.shape["blk"] == 16 and mesh.shape["row"] == 2
    in_specs = (P(AXES, None), P(AXES, None), P(), P(), P())
    out_specs = (P(AXES, None), P(AXES, None))
    return jax.shard_map(
        small_slice if small else large_slice,
        mesh=mesh,
        in_specs=in_specs,
        out_specs=out_specs,
        check_vma=False,
    )
```

```python
import functools

import jax
import jax.numpy as jnp
from jax import lax
from jax.experimental import pallas as pl
from jax.experimental.pallas import tpu as pltpu
from jax.sharding import PartitionSpec as P

highest = lax.Precision.HIGHEST
root_five = 2.23606797749979
tiny = 1e-30
AXES = ("blk", "row")
NT = (((1,), (1,)), ((), ()))
NN = (((1,), (0,)), ((), ()))


def split(value):
    high = value.astype(jnp.bfloat16)
    low = (value - high.astype(jnp.float32)).astype(jnp.bfloat16)
    return high, low


def dot3(left, right, dims):
    left_high, left_low = left
    right_high, right_low = right
    product = functools.partial(
        lax.dot_general, dimension_numbers=dims, preferred_element_type=jnp.float32
    )
    return (
        product(left_high, right_low) + product(left_low, right_high) + product(left_high, right_high)
    )


def dot6(left, right, dims):
    return lax.dot_general(left, right, dims, precision=highest, preferred_element_type=jnp.float32)


def matern(row_feats, row_norms, col_feats, col_norms):
    five_squared = dot6(row_feats, col_feats, NT) + row_norms + col_norms
    five_squared = jnp.maximum(five_squared, tiny)
    scaled = five_squared * lax.rsqrt(five_squared)
    return (1.0 + scaled + five_squared * (1.0 / 3.0)) * jnp.exp(-scaled)


def lane_norms(feats):
    ones = jnp.full((8, feats.shape[1]), 5.0, jnp.float32)
    return dot6(ones, feats * feats, NT)[0:1, :]


def tile_kernel(index_ref, scalar_ref, *refs):
    pieces = refs[:8]
    probes_ref, gram_ref, send_ref, keep_ref, cross_ref, all_ref, query_ref = refs[8:]
    line_rows, feature_count = pieces[0].shape
    rank = gram_ref.shape[0]
    local_rows = cross_ref.shape[0]
    amplitude = scalar_ref[0]
    nugget = scalar_ref[1]
    for position, piece in enumerate(pieces):
        all_ref[position * line_rows : (position + 1) * line_rows, :] = piece[:, :]

    def pick(step, carry):
        query_ref[pl.ds(step, 1), :] = all_ref[pl.ds(index_ref[step], 1), :]
        return carry

    lax.fori_loop(0, rank, pick, 0, unroll=8)
    pivot_feats = query_ref[:rank, :]
    line_feats = pieces[0][:, :]
    query_ref[rank:, :] = line_feats
    query = query_ref[:, :]
    query_norms = 5.0 * jnp.sum(query * query, axis=1, keepdims=True)
    query_scaled = -10.0 * query
    pivot_norms = lane_norms(pivot_feats)
    line_norms = lane_norms(line_feats)
    probes = split(probes_ref[:, :])
    total = None
    line_cross = None
    for position, piece in enumerate(pieces):
        feats = piece[:, :]
        tile = matern(query_scaled, query_norms, feats, lane_norms(feats))
        halves = split(tile)
        part = dot3((halves[0][:rank], halves[1][:rank]), halves, NT)
        total = part if total is None else total + part
        if position == 0:
            line_cross = tile[:rank, :]
        own = feats[:local_rows, :]
        own_norms = 5.0 * jnp.sum(own * own, axis=1, keepdims=True)
        own_tile = matern(-10.0 * own, own_norms, line_feats, line_norms)
        rows = dot3(split(own_tile), probes, NN)
        if position < 4:
            keep_ref[position * local_rows : (position + 1) * local_rows, :] = rows
        else:
            send_ref[(position - 4) * local_rows : (position - 3) * local_rows, :] = rows
        if position == 0:
            cross_ref[:, :] = amplitude * matern(-10.0 * own, own_norms, pivot_feats, pivot_norms)
    inner = matern(query_scaled[:rank], query_norms[:rank], pivot_feats, pivot_norms)
    square = amplitude * amplitude
    gram_ref[:, :] = (nugget * amplitude) * inner + square * total[:, :rank]
    mixed = square * total[:, rank:] + (nugget * amplitude) * line_cross
    projected = dot3(split(mixed), probes, NN)
    keep_ref[4 * local_rows :, :] = projected
    send_ref[4 * local_rows :, :] = projected


LANES, SUB, PANEL = 128, 8, 32

def reciprocal(value):
    guess = pl.reciprocal(value, approx=True)
    return guess * (2.0 - value * guess)

def panel_rows(matrix_ref, start):
    tiles = matrix_ref.shape[1] // LANES
    home = start // LANES
    sublane = lax.broadcasted_iota(jnp.int32, (SUB, LANES), 0)
    lane = lax.broadcasted_iota(jnp.int32, (SUB, LANES), 1)
    groups = [
        [matrix_ref[start + SUB * g : start + SUB * (g + 1), LANES * t : LANES * (t + 1)] for t in range(tiles)]
        for g in range(PANEL // SUB)
    ]
    for own in range(PANEL // SUB):
        base = (start + SUB * own) % LANES
        columns = [
            [jnp.broadcast_to(group[home][:, base + j : base + j + 1], (SUB, LANES)) for j in range(SUB)]
            for group in groups
        ]
        rows = list(groups[own])
        local = list(columns[own])
        for j in range(SUB):
            here = sublane == j
            inverse = reciprocal(jnp.broadcast_to(local[j][j : j + 1, :], (SUB, LANES)))
            factor = local[j]
            for c in range(j + 1, SUB):
                scaled = jnp.broadcast_to(local[c][j : j + 1, :], (SUB, LANES)) * inverse
                local[c] = jnp.where(here, scaled, local[c] - factor * scaled)
            unit = jnp.where(here, 1.0, 0.0)
            rows[home] = jnp.where(lane == base + j, unit, rows[home])
            for t in range(tiles):
                scaled = jnp.broadcast_to(rows[t][j : j + 1, :], (SUB, LANES)) * inverse
                rows[t] = jnp.where(here, scaled, rows[t] - factor * scaled)
        groups[own] = rows
        inside = (lane >= base) & (lane < base + SUB)
        for g in range(PANEL // SUB):
            if g != own:
                for t in range(tiles):
                    value = groups[g][t]
                    if t == home:
                        value = jnp.where(inside, 0.0, value)
                    for j in range(SUB):
                        value = value - columns[g][j] * jnp.broadcast_to(rows[t][j : j + 1, :], (SUB, LANES))
                    groups[g][t] = value
    return jnp.concatenate([jnp.concatenate(group, axis=1) for group in groups], axis=0)

def eliminate(matrix_ref, start):
    size = matrix_ref.shape[0]
    home = start // LANES
    solved = panel_rows(matrix_ref, start)
    matrix_ref[start : start + PANEL, :] = solved
    before = start % LANES
    pad = [jnp.zeros((before, size), jnp.float32)] * (before > 0) + [solved] + [jnp.zeros((LANES - PANEL - before, size), jnp.float32)] * (before + PANEL < LANES)
    padded = jnp.concatenate(pad, axis=0) if len(pad) > 1 else solved
    after = start + PANEL
    chunks = [(after, after + PANEL), (after + PANEL, size), (0, start)]
    for low, high in chunks:
        if low < high and low < size:
            block = matrix_ref[low:high, LANES * home : LANES * (home + 1)]
            update = dot6(block, padded, NN)
            lane = lax.broadcasted_iota(jnp.int32, block.shape, 1)
            inside = (lane >= before) & (lane < before + PANEL)
            for t in range(size // LANES):
                value = jnp.where(inside, 0.0, block) if t == home else matrix_ref[low:high, LANES * t : LANES * (t + 1)]
                matrix_ref[low:high, LANES * t : LANES * (t + 1)] = value - update[:, LANES * t : LANES * (t + 1)]


def invert_kernel(gram_ref, out_ref, *, first, last):
    out_ref[:, :] = gram_ref[:, :]
    for panel in range(first, last):
        eliminate(out_ref, panel * PANEL)


def weight_kernel(gram_ref, cross_ref, out_ref, work_ref, *, first, last):
    invert_kernel(gram_ref, work_ref, first=first, last=last)
    out_ref[:, :] = dot6(cross_ref[:, :], work_ref[:, :], NN)


def final_kernel(scalar_ref, kept_ref, arrived_ref, probes_ref, weight_ref, product_ref, out_ref):
    local_rows = probes_ref.shape[0]
    nugget = scalar_ref[1]
    kernel_probes = kept_ref[:local_rows, :] + arrived_ref[:local_rows, :]
    projected = kept_ref[2 * local_rows :, :] + arrived_ref[local_rows:, :]
    product = scalar_ref[0] * kernel_probes + nugget * probes_ref[:, :]
    product_ref[:, :] = product
    correction = dot6(weight_ref[:, :], projected, NN)
    out_ref[:, :] = (product - correction) * (1.0 / nugget)


def exchanged(value, mask, count):
    return lax.ppermute(value, AXES, [(i, i ^ mask) for i in range(count)])


def small_slice(features, probes, outputscale, noise, pivots):
    local_rows, probe_count = probes.shape
    feature_count = features.shape[1]
    rank = pivots.shape[0]
    row_count = lax.axis_size("row")
    count = lax.axis_size("blk") * row_count
    flat_index = lax.axis_index("blk") * row_count + lax.axis_index("row")
    step_x, step_core, step_y, step_z = 1, row_count, 2 * row_count, 4 * row_count
    send = functools.partial(exchanged, count=count)

    owner = (pivots // local_rows) ^ flat_index
    slot = ((owner // step_y) & 1) + 2 * (owner & 1) + 4 * ((owner // step_core) & 1)
    index = (slot * 4 + owner // step_z) * local_rows + pivots % local_rows

    packed = jnp.concatenate([features, probes], axis=1)
    line = [packed] + [send(packed, step_z * step) for step in (1, 2, 3)]
    line_feats = jnp.concatenate([part[:, :feature_count] for part in line], axis=0)
    line_probes = jnp.concatenate([part[:, feature_count:] for part in line], axis=0)
    pieces = [line_feats] + [send(line_feats, mask) for mask in (step_y, step_x, step_x + step_y)]
    pieces = pieces + [send(piece, step_core) for piece in pieces]

    scalars = jnp.concatenate([outputscale, noise])
    vmem = pl.BlockSpec(memory_space=pltpu.VMEM)
    smem = pl.BlockSpec(memory_space=pltpu.SMEM)
    half = 4 * local_rows + rank
    gram, outgoing, kept, cross = pl.pallas_call(
        tile_kernel,
        out_shape=(
            jax.ShapeDtypeStruct((rank, rank), jnp.float32),
            jax.ShapeDtypeStruct((half, probe_count), jnp.float32),
            jax.ShapeDtypeStruct((half, probe_count), jnp.float32),
            jax.ShapeDtypeStruct((local_rows, rank), jnp.float32),
        ),
        in_specs=[smem, smem] + [vmem] * 9,
        out_specs=(vmem,) * 4,
        scratch_shapes=[
            pltpu.VMEM((8 * 4 * local_rows, feature_count), jnp.float32),
            pltpu.VMEM((rank + 4 * local_rows, feature_count), jnp.float32),
        ],
        name="tiles",
    )(index, scalars, *pieces, line_probes)

    panels = rank // PANEL
    cuts = (panels * 3 // 8, panels * 6 // 8)
    cost = pl.CostEstimate(flops=4 * rank**3, bytes_accessed=8 * rank**2, transcendentals=0)
    matrix = jax.ShapeDtypeStruct((rank, rank), jnp.float32)

    def steps(value, first, last):
        return pl.pallas_call(
            functools.partial(invert_kernel, first=first, last=last),
            out_shape=matrix,
            in_specs=[vmem],
            out_specs=vmem,
            cost_estimate=cost,
            name="steps",
        )(value)

    arrived = send(outgoing, step_core)
    inverse = steps(gram, 0, cuts[0])
    inverse, arrived = lax.optimization_barrier((inverse, arrived))
    kept = kept + arrived
    arrived = send(kept[2 * local_rows :], step_x)
    inverse = steps(inverse, cuts[0], cuts[1])
    inverse, arrived = lax.optimization_barrier((inverse, arrived))
    kept = jnp.concatenate(
        [
            kept[: 2 * local_rows] + arrived[: 2 * local_rows],
            kept[4 * local_rows :] + arrived[2 * local_rows :],
        ]
    )
    arrived = send(kept[local_rows:], step_y)
    weight = pl.pallas_call(
        functools.partial(weight_kernel, first=cuts[1], last=panels),
        out_shape=jax.ShapeDtypeStruct(cross.shape, jnp.float32),
        in_specs=[vmem] * 2,
        out_specs=vmem,
        scratch_shapes=[pltpu.VMEM((rank, rank), jnp.float32)],
        cost_estimate=cost,
        name="weight",
    )(inverse, cross)
    output = jax.ShapeDtypeStruct(probes.shape, jnp.float32)
    return pl.pallas_call(
        final_kernel,
        out_shape=(output, output),
        in_specs=[smem] + [vmem] * 4,
        out_specs=(vmem, vmem),
        name="final",
    )(scalars, kept, arrived, probes, weight)


def plain_tile(row_feats, col_feats):
    row_norms = 5.0 * jnp.sum(row_feats * row_feats, axis=1)[:, None]
    col_norms = 5.0 * jnp.sum(col_feats * col_feats, axis=1)[None, :]
    return matern(-10.0 * row_feats, row_norms, col_feats, col_norms)


def large_slice(features, probes, outputscale, noise, pivots):
    dot = functools.partial(jnp.dot, precision=highest, preferred_element_type=jnp.float32)
    amplitude = outputscale[0]
    nugget = noise[0]
    all_feats = lax.all_gather(features, AXES, axis=0, tiled=True)
    all_probes = lax.all_gather(probes, AXES, axis=0, tiled=True)
    product = amplitude * dot(plain_tile(features, all_feats), all_probes) + nugget * probes
    pivot_feats = all_feats[pivots]
    cross = amplitude * plain_tile(features, pivot_feats)
    inner = amplitude * plain_tile(pivot_feats, pivot_feats)
    gram, projected = lax.psum((dot(cross.T, cross), dot(cross.T, product)), AXES)
    factor = jnp.linalg.cholesky(nugget * inner + gram)
    coefficients = jax.scipy.linalg.cho_solve((factor, True), projected)
    return product, (product - dot(cross, coefficients)) / nugget


def solution(mesh):
    small = mesh.shape["blk"] == 16 and mesh.shape["row"] == 2
    in_specs = (P(AXES, None), P(AXES, None), P(), P(), P())
    out_specs = (P(AXES, None), P(AXES, None))
    return jax.shard_map(
        small_slice if small else large_slice,
        mesh=mesh,
        in_specs=in_specs,
        out_specs=out_specs,
        check_vma=False,
    )
```

```python
import functools

import jax
import jax.numpy as jnp
from jax import lax
from jax.experimental import pallas as pl
from jax.experimental.pallas import tpu as pltpu
from jax.sharding import PartitionSpec as P

highest = lax.Precision.HIGHEST
root_five = 2.23606797749979
tiny = 1e-30
AXES = ("blk", "row")
NT = (((1,), (1,)), ((), ()))
NN = (((1,), (0,)), ((), ()))
vmem = pl.BlockSpec(memory_space=pltpu.VMEM)
smem = pl.BlockSpec(memory_space=pltpu.SMEM)


def split(value, count=2):
    parts = []
    for _ in range(count):
        part = value.astype(jnp.bfloat16)
        parts.append(part)
        if len(parts) < count:
            value = value - part.astype(jnp.float32)
    return parts


def dot(left, right, dims):
    return lax.dot_general(left, right, dims, preferred_element_type=jnp.float32)


def dot6(left, right, dims):
    return lax.dot_general(left, right, dims, precision=highest, preferred_element_type=jnp.float32)


def dot3(left, right, dims):
    return dot(left[0], right[1], dims) + dot(left[1], right[0], dims) + dot(left[0], right[0], dims)


def row_side(value):
    high, mid = split(value)
    return jnp.concatenate([mid, mid, high, high], axis=1)


def col_side(value):
    high, mid = split(value)
    return jnp.concatenate([mid, high, mid, high], axis=1)


def matern(row_wide, row_norms, col_wide, col_norms):
    five_squared = dot(row_wide, col_wide, NT) + row_norms + col_norms
    five_squared = jnp.maximum(five_squared, tiny)
    scaled = five_squared * lax.rsqrt(five_squared)
    return (1.0 + scaled + five_squared * (1.0 / 3.0)) * jnp.exp(-scaled)


def sums(feats):
    return 5.0 * jnp.sum(feats * feats, axis=1, keepdims=True)


def flipped(column):
    return jnp.transpose(jnp.broadcast_to(column, (column.shape[0], 128)))[0:1, :]


def tile_kernel(index_ref, scale_ref, noise_ref, *refs):
    pieces = refs[:8]
    (probes_ref, gram_ref, send_ref, keep_ref, cross_ref, all_ref, query_ref,
     wide_ref, high_ref, low_ref) = refs[8:]
    line_rows, feature_count = pieces[0].shape
    rank = gram_ref.shape[0]
    local_rows = cross_ref.shape[0]
    amplitude = scale_ref[0]
    nugget = noise_ref[0]
    for position, piece in enumerate(pieces):
        all_ref[position * line_rows : (position + 1) * line_rows, :] = piece[:, :]
    def pick(step, carry):
        query_ref[pl.ds(step, 1), :] = all_ref[pl.ds(index_ref[step], 1), :]
        return carry
    lax.fori_loop(0, rank, pick, 0, unroll=8)
    pivot_feats = query_ref[:, :]
    line_feats = pieces[0][:, :]
    pivot_sums = sums(pivot_feats)
    line_sums = sums(line_feats)
    query_sums = jnp.concatenate([pivot_sums, line_sums], axis=0)
    pivot_flipped = flipped(pivot_sums)
    line_flipped = flipped(line_sums)
    wide_ref[:rank, :] = row_side(-10.0 * pivot_feats)
    wide_ref[rank:, :] = row_side(-10.0 * line_feats)
    line_wide = col_side(line_feats)
    pivot_wide = col_side(pivot_feats)
    probes = split(probes_ref[:, :])
    own = jnp.concatenate([piece[:local_rows, :] for piece in pieces], axis=0)
    own_wide = row_side(-10.0 * own)
    own_sums = sums(own)
    rows = dot3(split(matern(own_wide, own_sums, line_wide, line_flipped)), probes, NN)
    keep_ref[: 4 * local_rows, :] = rows[: 4 * local_rows, :]
    send_ref[: 4 * local_rows, :] = rows[4 * local_rows :, :]
    cross_ref[:, :] = amplitude * matern(own_wide[:local_rows], own_sums[:local_rows], pivot_wide, pivot_flipped)
    for position, piece in enumerate(pieces):
        feats = piece[:, :]
        feat_sums = sums(feats) if position else line_sums
        wide = [wide_ref[:rank, :], wide_ref[rank:, :]]; col = col_side(feats) if position else line_wide; fl=flipped(feat_sums)
        tile = jnp.concatenate([matern(wide[0], pivot_sums, col, fl), matern(wide[1], line_sums, col, fl)], axis=0)
        span = slice(position * line_rows, (position + 1) * line_rows)
        high, low = split(tile)
        high_ref[:, span] = high
        low_ref[:, span] = low
        if position == 0:
            line_cross = tile[:rank, :]
    inner = matern(wide_ref[:rank, :], pivot_sums, pivot_wide, pivot_flipped)
    square = amplitude * amplitude
    left_high, left_low = high_ref[:, :], low_ref[:, :]
    total = dot3((left_high, left_low), (left_high[:rank], left_low[:rank]), NT)
    gram_ref[:, :] = (nugget * amplitude) * inner + square * total[:rank, :]
    mixed = square * total[rank:, :] + (nugget * amplitude) * jnp.transpose(line_cross)
    projected = dot3(split(jnp.transpose(mixed)), probes, NN)
    keep_ref[4 * local_rows :, :] = projected
    send_ref[4 * local_rows :, :] = projected


LANES, SUB, PANEL = 128, 8, 32

def reciprocal(value):
    guess = pl.reciprocal(value, approx=True)
    return guess * (2.0 - value * guess)

def panel_rows(matrix_ref, start):
    tiles = matrix_ref.shape[1] // LANES
    home = start // LANES
    sublane = lax.broadcasted_iota(jnp.int32, (SUB, LANES), 0)
    lane = lax.broadcasted_iota(jnp.int32, (SUB, LANES), 1)
    groups = [
        [matrix_ref[start + SUB * g : start + SUB * (g + 1), LANES * t : LANES * (t + 1)] for t in range(tiles)]
        for g in range(PANEL // SUB)
    ]
    for own in range(PANEL // SUB):
        base = (start + SUB * own) % LANES
        columns = [
            [jnp.broadcast_to(group[home][:, base + j : base + j + 1], (SUB, LANES)) for j in range(SUB)]
            for group in groups
        ]
        rows = list(groups[own])
        local = list(columns[own])
        for j in range(SUB):
            here = sublane == j
            inverse = reciprocal(jnp.broadcast_to(local[j][j : j + 1, :], (SUB, LANES)))
            factor = local[j]
            for c in range(j + 1, SUB):
                scaled = jnp.broadcast_to(local[c][j : j + 1, :], (SUB, LANES)) * inverse
                local[c] = jnp.where(here, scaled, local[c] - factor * scaled)
            unit = jnp.where(here, 1.0, 0.0)
            rows[home] = jnp.where(lane == base + j, unit, rows[home])
            for t in range(tiles):
                scaled = jnp.broadcast_to(rows[t][j : j + 1, :], (SUB, LANES)) * inverse
                rows[t] = jnp.where(here, scaled, rows[t] - factor * scaled)
        groups[own] = rows
        inside = (lane >= base) & (lane < base + SUB)
        for g in range(PANEL // SUB):
            if g != own:
                for t in range(tiles):
                    value = groups[g][t]
                    if t == home:
                        value = jnp.where(inside, 0.0, value)
                    for j in range(SUB):
                        value = value - columns[g][j] * jnp.broadcast_to(rows[t][j : j + 1, :], (SUB, LANES))
                    groups[g][t] = value
    return jnp.concatenate([jnp.concatenate(group, axis=1) for group in groups], axis=0)

def eliminate(matrix_ref, start):
    size = matrix_ref.shape[0]
    home = start // LANES
    solved = panel_rows(matrix_ref, start)
    matrix_ref[start : start + PANEL, :] = solved
    before = start % LANES
    pad = [jnp.zeros((before, size), jnp.float32)] * (before > 0) + [solved] + [jnp.zeros((LANES - PANEL - before, size), jnp.float32)] * (before + PANEL < LANES)
    padded = jnp.concatenate(pad, axis=0) if len(pad) > 1 else solved
    after = start + PANEL
    chunks = [(after, after + PANEL), (after + PANEL, size), (0, start)]
    for low, high in chunks:
        if low < high and low < size:
            block = matrix_ref[low:high, LANES * home : LANES * (home + 1)]
            update = dot6(block, padded, NN)
            lane = lax.broadcasted_iota(jnp.int32, block.shape, 1)
            inside = (lane >= before) & (lane < before + PANEL)
            for t in range(size // LANES):
                value = jnp.where(inside, 0.0, block) if t == home else matrix_ref[low:high, LANES * t : LANES * (t + 1)]
                matrix_ref[low:high, LANES * t : LANES * (t + 1)] = value - update[:, LANES * t : LANES * (t + 1)]


def invert_kernel(gram_ref, out_ref, *, first, last):
    out_ref[:, :] = gram_ref[:, :]
    for panel in range(first, last):
        eliminate(out_ref, panel * PANEL)


def weight_kernel(gram_ref, cross_ref, out_ref, work_ref, *, first, last):
    invert_kernel(gram_ref, work_ref, first=first, last=last)
    out_ref[:, :] = dot6(cross_ref[:, :], work_ref[:, :], NN)


def final_kernel(scale_ref, noise_ref, kept_ref, arrived_ref, probes_ref, weight_ref, product_ref, out_ref):
    local_rows = probes_ref.shape[0]
    nugget = noise_ref[0]
    kernel_probes = kept_ref[:local_rows, :] + arrived_ref[:local_rows, :]
    projected = kept_ref[2 * local_rows :, :] + arrived_ref[local_rows:, :]
    product = scale_ref[0] * kernel_probes + nugget * probes_ref[:, :]
    product_ref[:, :] = product
    correction = dot6(weight_ref[:, :], projected, NN)
    out_ref[:, :] = (product - correction) * (1.0 / nugget)


def near(value):
    return pltpu.with_memory_space_constraint(value, pltpu.VMEM)


def assemble_kernel(*refs):
    parts, (feats_ref, probes_ref) = refs[:4], refs[4:]
    rows = parts[0].shape[0]
    feature_count = feats_ref.shape[1]
    for position, part in enumerate(parts):
        span = slice(position * rows, (position + 1) * rows)
        feats_ref[span, :] = part[:, :feature_count]
        probes_ref[span, :] = part[:, feature_count:]


def exchanged(value, mask, count):
    return lax.ppermute(value, AXES, [(i, i ^ mask) for i in range(count)])


def small_slice(features, probes, outputscale, noise, pivots):
    local_rows, probe_count = probes.shape
    feature_count = features.shape[1]
    rank = pivots.shape[0]
    row_count = lax.axis_size("row")
    count = lax.axis_size("blk") * row_count
    flat_index = lax.axis_index("blk") * row_count + lax.axis_index("row")
    step_x, step_core, step_y, step_z = 1, row_count, 2 * row_count, 4 * row_count
    send = functools.partial(exchanged, count=count)

    owner = (pivots // local_rows) ^ flat_index
    slot = ((owner // step_y) & 1) + 2 * (owner & 1) + 4 * ((owner // step_core) & 1)
    index = (slot * 4 + owner // step_z) * local_rows + pivots % local_rows

    packed = jnp.concatenate([features, probes], axis=1)
    line = [packed] + [send(packed, step_z * step) for step in (1, 2, 3)]
    line_rows = 4 * local_rows
    line_feats, line_probes = pl.pallas_call(
        assemble_kernel,
        out_shape=(
            pltpu.VMEM((line_rows, feature_count), jnp.float32),
            pltpu.VMEM((line_rows, probe_count), jnp.float32),
        ),
        in_specs=[vmem] * 4,
        out_specs=(vmem,) * 2,
        name="assemble",
    )(*[near(part) for part in line])
    arrived = [send(line_feats, mask) for mask in (step_y, step_x, step_x + step_y)]
    arrived[0], index = lax.optimization_barrier((arrived[0], index))
    pieces = [line_feats] + arrived
    pieces = pieces + [send(piece, step_core) for piece in pieces]

    half = line_rows + rank
    wide = line_rows + rank
    gram, outgoing, kept, cross = pl.pallas_call(
        tile_kernel,
        out_shape=(
            pltpu.VMEM((rank, rank), jnp.float32),
            pltpu.VMEM((half, probe_count), jnp.float32),
            pltpu.VMEM((half, probe_count), jnp.float32),
            pltpu.VMEM((local_rows, rank), jnp.float32),
        ),
        in_specs=[smem] * 3 + [vmem] * 9,
        out_specs=(vmem,) * 4,
        scratch_shapes=[
            pltpu.VMEM((8 * line_rows, feature_count), jnp.float32),
            pltpu.VMEM((rank, feature_count), jnp.float32),
            pltpu.VMEM((wide, 4 * feature_count), jnp.bfloat16),
            pltpu.VMEM((wide, 8 * line_rows), jnp.bfloat16),
            pltpu.VMEM((wide, 8 * line_rows), jnp.bfloat16),
        ],
        name="tiles",
    )(index, outputscale, noise, *[near(piece) for piece in pieces], near(line_probes))

    panels = rank // PANEL
    cuts = (panels * 3 // 8, panels * 6 // 8)
    cost = pl.CostEstimate(flops=4 * rank**3, bytes_accessed=8 * rank**2, transcendentals=0)
    matrix = pltpu.VMEM((rank, rank), jnp.float32)

    def steps(value, first, last):
        return pl.pallas_call(
            functools.partial(invert_kernel, first=first, last=last),
            out_shape=matrix,
            in_specs=[vmem],
            out_specs=vmem,
            cost_estimate=cost,
            name="steps",
        )(near(value))

    arrived = send(outgoing, step_core)
    inverse = steps(gram, 0, cuts[0])
    inverse, arrived = lax.optimization_barrier((inverse, arrived))
    kept = kept + arrived
    arrived = send(kept[2 * local_rows :], step_x)
    inverse = steps(inverse, cuts[0], cuts[1])
    inverse, arrived = lax.optimization_barrier((inverse, arrived))
    kept = jnp.concatenate(
        [
            kept[: 2 * local_rows] + arrived[: 2 * local_rows],
            kept[4 * local_rows :] + arrived[2 * local_rows :],
        ]
    )
    arrived = send(kept[local_rows:], step_y)
    weight = pl.pallas_call(
        functools.partial(weight_kernel, first=cuts[1], last=panels),
        out_shape=pltpu.VMEM(cross.shape, jnp.float32),
        in_specs=[vmem] * 2,
        out_specs=vmem,
        scratch_shapes=[pltpu.VMEM((rank, rank), jnp.float32)],
        cost_estimate=cost,
        name="weight",
    )(near(inverse), near(cross))
    output = jax.ShapeDtypeStruct(probes.shape, jnp.float32)
    return pl.pallas_call(
        final_kernel,
        out_shape=(output, output),
        in_specs=[smem] * 2 + [vmem] * 4,
        out_specs=(vmem, vmem),
        name="final",
    )(outputscale, noise, near(kept), near(arrived), probes, near(weight))


def plain_tile(row_feats, col_feats):
    row_norms = jnp.sum(row_feats * row_feats, axis=1)[:, None]
    col_norms = jnp.sum(col_feats * col_feats, axis=1)[None, :]
    inner = dot6(row_feats, col_feats, NT)
    scaled = root_five * jnp.sqrt(jnp.maximum(row_norms + col_norms - 2.0 * inner, 0.0))
    return (1.0 + scaled + scaled * scaled / 3.0) * jnp.exp(-scaled)


def large_slice(features, probes, outputscale, noise, pivots):
    dot = functools.partial(jnp.dot, precision=highest, preferred_element_type=jnp.float32)
    amplitude = outputscale[0]
    nugget = noise[0]
    all_feats = lax.all_gather(features, AXES, axis=0, tiled=True)
    all_probes = lax.all_gather(probes, AXES, axis=0, tiled=True)
    product = amplitude * dot(plain_tile(features, all_feats), all_probes) + nugget * probes
    pivot_feats = all_feats[pivots]
    cross = amplitude * plain_tile(features, pivot_feats)
    inner = amplitude * plain_tile(pivot_feats, pivot_feats)
    gram, projected = lax.psum((dot(cross.T, cross), dot(cross.T, product)), AXES)
    factor = jnp.linalg.cholesky(nugget * inner + gram)
    coefficients = jax.scipy.linalg.cho_solve((factor, True), projected)
    return product, (product - dot(cross, coefficients)) / nugget


def solution(mesh):
    small = mesh.shape["blk"] == 16 and mesh.shape["row"] == 2
    in_specs = (P(AXES, None), P(AXES, None), P(), P(), P())
    out_specs = (P(AXES, None), P(AXES, None))
    return jax.shard_map(
        small_slice if small else large_slice,
        mesh=mesh,
        in_specs=in_specs,
        out_specs=out_specs,
        check_vma=False,
    )
```
